32 devices in a mesh: trial: 4 (over x, core), north: 2 (over y), east: 4 (over z).
Axes of the slice: x: 2, y: 2, z: 4, core: 2. Of those that a mesh axis runs over, the one named last changes fastest.
Arguments:
- pair_state: bfloat16 [192, 48, 128], P(('trial', 'north'), 'east'), parts along dimension 0, may hold values from -6 to 6
- in_gain: float32 [128], replicated, may hold values from 0.25 to 1.75
- left_weight: bfloat16 [512, 128], P('trial'), parts along dimension 0, may hold values from -0.5 to 0.5
- right_weight: bfloat16 [512, 128], P('trial'), parts along dimension 0, may hold values from -0.5 to 0.5
- left_gate: bfloat16 [512, 128], P('trial'), parts along dimension 0, may hold values from -0.5 to 0.5
- right_gate: bfloat16 [512, 128], P('trial'), parts along dimension 0, may hold values from -0.5 to 0.5
- mid_gain: float32 [128], replicated, may hold values from 0.25 to 1.75
- out_weight: bfloat16 [512, 128], P('trial'), parts along dimension 0, may hold values from -0.5 to 0.5
- out_gate: bfloat16 [512, 128], P('trial'), parts along dimension 0, may hold values from -0.5 to 0.5
Outputs:
- triangle_out: bfloat16 [192, 48, 128], P(('trial', 'north'), 'east'), parts along dimension 0
The draws below stay inside these ranges and needn't reach their ends.
There are 4 independent parts, one for each index of `trial`. The reference program is written for one: setup_inputs(seed, part) draws one part's arguments, and reference() takes and returns one part's arrays. A program takes and returns all parts, laid end to end along the dimension named above; an argument that names none is the same for every part. Nothing has to cross between parts.
All inputs are finite; a program needn't handle non-finite values.
Results may differ from the reference program's by a relative error of at most 0.015.
Values may be sent and summed in bfloat16 or wider, within the bound.
A program may use at most 64 MiB of HBM per device.

```python
import jax
import jax.numpy as jnp
from jax import lax

RESIDUES = 48
PAIR_WIDTH = 128
MIX_WIDTH = 128


def block_scale(own_key, shape, pieces, low, top_value):
    def one(axis_at, blocks):
        draws = jax.random.uniform(jax.random.fold_in(jax.random.fold_in(own_key, 6), axis_at), (blocks,), jnp.float32, low / len(pieces), top_value / len(pieces))
        return jnp.repeat(jnp.exp(draws), shape[axis_at] // blocks).reshape((-1,) + (1,) * (len(shape) - axis_at - 1))

    level = one(*pieces[0])
    for cut in pieces[1:]:
        level = level * one(*cut)
    return level


def scatter_about(stream_key, shape, spread, reach, shards=(), kind=jnp.bfloat16):
    values = spread * jax.random.normal(stream_key, shape, jnp.float32)
    if shards:
        values = values * block_scale(stream_key, shape, shards, -0.22, 0.18)
    return jnp.clip(values, -reach, reach).astype(kind)


def setup_inputs(seed: int = 0, part: int = 0) -> dict:
    keys = jax.random.split(jax.random.key(seed), 10)
    own_keys = jax.random.split(jax.random.fold_in(keys[9], part), 10)
    pair_state = scatter_about(own_keys[0], (RESIDUES, RESIDUES, PAIR_WIDTH), 1.0, 6.0, ((0, 2), (1, 4)))
    in_gain = jnp.clip(1.0 + 0.15 * jax.random.normal(keys[1], (PAIR_WIDTH,), jnp.float32), 0.25, 1.75)
    left_weight = scatter_about(own_keys[2], (PAIR_WIDTH, MIX_WIDTH), PAIR_WIDTH ** -0.5, 0.5)
    right_weight = scatter_about(own_keys[3], (PAIR_WIDTH, MIX_WIDTH), PAIR_WIDTH ** -0.5, 0.5)
    left_gate = scatter_about(own_keys[4], (PAIR_WIDTH, MIX_WIDTH), PAIR_WIDTH ** -0.5, 0.5)
    right_gate = scatter_about(own_keys[5], (PAIR_WIDTH, MIX_WIDTH), PAIR_WIDTH ** -0.5, 0.5)
    mid_gain = jnp.clip(1.0 + 0.15 * jax.random.normal(keys[6], (MIX_WIDTH,), jnp.float32), 0.25, 1.75)
    out_weight = scatter_about(own_keys[7], (MIX_WIDTH, PAIR_WIDTH), MIX_WIDTH ** -0.5, 0.5)
    out_gate = scatter_about(own_keys[8], (PAIR_WIDTH, PAIR_WIDTH), PAIR_WIDTH ** -0.5, 0.5)
    return {"pair_state": pair_state, "in_gain": in_gain, "left_weight": left_weight, "right_weight": right_weight, "left_gate": left_gate, "right_gate": right_gate, "mid_gain": mid_gain, "out_weight": out_weight, "out_gate": out_gate}


def norm_channels(values, channel_gain):
    centred = values - lax.optimization_barrier(jnp.mean(values, axis=-1, keepdims=True))
    return centred * lax.rsqrt(lax.optimization_barrier(jnp.mean(centred * centred, axis=-1, keepdims=True)) + 1e-05) * channel_gain

def make_factors(pair_in, in_gain, left_weight, right_weight, left_gate, right_gate):
    ready = norm_channels(pair_in.astype(jnp.float32), in_gain).astype(jnp.bfloat16)
    ready = lax.optimization_barrier(ready)
    left = jnp.einsum('ijc,cd->ijd', ready.astype(jnp.float32), left_weight.astype(jnp.float32))
    left = left * jax.nn.sigmoid(jnp.einsum('ijc,cd->ijd', ready.astype(jnp.float32), left_gate.astype(jnp.float32)))
    right = jnp.einsum('ijc,cd->ijd', ready.astype(jnp.float32), right_weight.astype(jnp.float32))
    right = right * jax.nn.sigmoid(jnp.einsum('ijc,cd->ijd', ready.astype(jnp.float32), right_gate.astype(jnp.float32)))
    return (ready, left.astype(jnp.bfloat16), right.astype(jnp.bfloat16))

def to_pair(mixed, ready, mid_gain, out_weight, out_gate):
    scaled = norm_channels(mixed.astype(jnp.float32), mid_gain).astype(jnp.bfloat16)
    scaled = lax.optimization_barrier(scaled)
    gate = jax.nn.sigmoid(jnp.einsum('ijc,cd->ijd', ready.astype(jnp.float32), out_gate.astype(jnp.float32)))
    return (jnp.einsum('ijd,dc->ijc', scaled.astype(jnp.float32), out_weight.astype(jnp.float32)) * gate).astype(jnp.bfloat16)

def reference(pair_state, in_gain, left_weight, right_weight, left_gate, right_gate, mid_gain, out_weight, out_gate):
    ready, left, right = make_factors(pair_state, in_gain, left_weight, right_weight, left_gate, right_gate)
    left, right = lax.optimization_barrier((left, right))

    def one_channel(pair_of):
        return (jnp.dot(pair_of[0], pair_of[1].T, preferred_element_type=jnp.float32) * RESIDUES ** (-0.5)).astype(jnp.bfloat16)
    mixed = jnp.moveaxis(lax.map(one_channel, (jnp.moveaxis(left, -1, 0), jnp.moveaxis(right, -1, 0))), 0, -1)
    mixed = lax.optimization_barrier(mixed)
    return to_pair(mixed, ready, mid_gain, out_weight, out_gate)
```

```python
import functools
import math

import jax
import jax.numpy as jnp
from jax import lax
from jax.experimental import pallas as pl
from jax.experimental.pallas import tpu as pltpu
from jax.sharding import PartitionSpec as P

MESH = pl.DeviceIdType.MESH


def norm_channels(values, gain):
    centred = values - jnp.mean(values, axis=-1, keepdims=True)
    return centred * lax.rsqrt(jnp.mean(centred * centred, axis=-1, keepdims=True) + 1e-05) * gain


def logistic(values):
    return 0.5 * jnp.tanh(0.5 * values) + 0.5


def dot(a, b):
    return jnp.dot(a, b, preferred_element_type=jnp.float32)


def tile_of(size, step, most):
    return max(t for t in range(step, most + 1, step) if size % t == 0)


def loop(count, body):
    if count == 1:
        body(0)
    else:
        pl.loop(0, count)(body)


def kernel(
    sizes,
    x_hbm, in_gain_hbm, lw_hbm, rw_hbm, lg_hbm, rg_hbm, mid_gain_hbm, ow_hbm, og_hbm,
    out_ref,
    xs, in_gain, lw, rw, lg, rg, mid_gain, ow, og,
    left, right, gate, sent, got,
    load_sem, pair_send, pair_recv, tile_send, tile_recv,
):
    N, E, R, C, IT, JT = sizes
    rows = R * C
    block = IT * JT
    n = lax.axis_index("north")
    e = lax.axis_index("east")

    barrier = pltpu.get_barrier_semaphore()
    for d in range(1, N):
        pl.semaphore_signal(barrier, inc=1, device_id={"north": lax.rem(n + d, N)}, device_id_type=MESH)
    for d in range(1, E):
        pl.semaphore_signal(barrier, inc=1, device_id={"east": lax.rem(e + d, E)}, device_id_type=MESH)

    loads = [pltpu.make_async_copy(x_hbm, xs.at[n], load_sem.at[0])]
    for at, (src, dst) in enumerate(
        (
            (in_gain_hbm, in_gain), (lw_hbm, lw), (lg_hbm, lg), (rw_hbm, rw),
            (rg_hbm, rg), (og_hbm, og), (mid_gain_hbm, mid_gain), (ow_hbm, ow),
        )
    ):
        loads.append(pltpu.make_async_copy(src, dst, load_sem.at[at + 1]))
    for load in loads:
        load.start()
    loads[0].wait()
    pl.semaphore_wait(barrier, N - 1 + E - 1)

    pair_copies = []
    for d in range(1, N):
        pair_copies.append(
            pltpu.make_async_remote_copy(
                xs.at[n], xs.at[n], pair_send.at[d], pair_recv.at[d],
                device_id={"north": lax.rem(n + d, N)}, device_id_type=MESH,
            )
        )
        pair_copies[-1].start()
    for load in loads[1:]:
        load.wait()

    def ready_rows(m, start):
        values = xs[m, pl.ds(start, block), :].astype(jnp.float32)
        return norm_channels(values, in_gain[...]).astype(jnp.bfloat16)

    def own(at):
        start = pl.multiple_of(at * block, block)
        ready = ready_rows(n, start)
        at_rows = pl.ds(start, block)
        left[at_rows, :] = dot(ready, lw[...]) * logistic(dot(ready, lg[...]))
        right[n, at_rows, :] = dot(ready, rw[...]) * logistic(dot(ready, rg[...]))
        gate[at_rows, :] = logistic(dot(ready, og[...]))

    loop(rows // block, own)

    def other(m):
        def body(at):
            start = pl.multiple_of(at * block, block)
            ready = ready_rows(m, start)
            right[m, pl.ds(start, block), :] = dot(ready, rw[...]) * logistic(dot(ready, rg[...]))

        loop(rows // block, body)

    def tile(slot, target):
        def one(at):
            it, jt = at // (C // JT), lax.rem(at, C // JT)
            first = target * C + jt * JT
            m, j = first // R, lax.rem(first, R)

            def step(k, sums):
                lines = left[pl.ds(pl.multiple_of(k * R + it * IT, 8), IT), :]
                return tuple(
                    sums[a] + lines * right[m, pl.ds(k * R + j + a, 1), :] for a in range(JT)
                )

            sums = lax.fori_loop(
                0, C, step, tuple(jnp.zeros((IT, left.shape[1]), jnp.float32) for _ in range(JT))
            )
            start = pl.multiple_of(at * block, block)
            sent[slot, pl.ds(start, block), :] = jnp.concatenate(sums, axis=0).astype(jnp.bfloat16)

        loop(rows // block, one)

    def tile_copy(slot, peer, landing):
        return pltpu.make_async_remote_copy(
            sent.at[slot], got.at[landing], tile_send.at[slot], tile_recv.at[landing],
            device_id={"east": peer}, device_id_type=MESH,
        )

    reach = R // C
    for s in range(E):
        if s == min(reach, E - 1):
            for d in range(1, N):
                m = lax.rem(n + N - d, N)
                pltpu.make_async_remote_copy(
                    xs.at[m], xs.at[m], pair_send.at[d], pair_recv.at[d],
                    device_id={"north": m}, device_id_type=MESH,
                ).wait_recv()
                other(m)
        target = lax.rem(n * reach + s, E)
        tile(s, target)

        @pl.when(target != e)
        def _():
            tile_copy(s, target, e).start()

    self_slot = lax.rem(e + N * E - n * reach, E)
    for d in range(1, E):
        peer = lax.rem(e + d, E)
        tile_copy(0, peer, peer).wait_recv()

    def finish(at):
        start = pl.multiple_of(at * block, block)
        total = sent[self_slot, pl.ds(start, block), :].astype(jnp.float32)
        for d in range(1, E):
            total += got[lax.rem(e + d, E), pl.ds(start, block), :].astype(jnp.float32)
        mixed = (total * (C * E) ** (-0.5)).astype(jnp.bfloat16).astype(jnp.float32)
        scaled = norm_channels(mixed, mid_gain[...]).astype(jnp.bfloat16)
        it, jt = at // (C // JT), at % (C // JT)
        gates = jnp.concatenate(
            [gate[pl.ds(pl.multiple_of((jt * JT + a) * R + it * IT, 8), IT), :] for a in range(JT)],
            axis=0,
        )
        out_ref[pl.ds(start, block), :] = (dot(scaled, ow[...]) * gates).astype(jnp.bfloat16)

    loop(rows // block, finish)

    for s in range(E):
        @pl.when(lax.rem(n * reach + s, E) != e)
        def _():
            tile_copy(s, lax.rem(n * reach + s, E), e).wait_send()
    for copy in pair_copies:
        copy.wait_send()


def local(N, E, pair_state, in_gain, lw, rw, lg, rg, mid_gain, ow, og):
    R, C, width = pair_state.shape
    mix = lw.shape[1]
    IT = tile_of(R, 8, 24)
    JT = tile_of(math.gcd(R, C), 1, 12)
    rows = R * C
    x = pair_state.transpose(1, 0, 2).reshape(rows, width)
    f32, bf16 = jnp.float32, jnp.bfloat16
    any_space = pl.BlockSpec(memory_space=pl.ANY)
    out = pl.pallas_call(
        functools.partial(kernel, (N, E, R, C, IT, JT)),
        out_shape=jax.ShapeDtypeStruct((rows, width), bf16),
        in_specs=[any_space] * 9,
        out_specs=pl.BlockSpec(memory_space=pltpu.VMEM),
        scratch_shapes=[
            pltpu.VMEM((N, rows, width), bf16),
            pltpu.VMEM((1, width), f32),
            pltpu.VMEM((width, mix), bf16),
            pltpu.VMEM((width, mix), bf16),
            pltpu.VMEM((width, mix), bf16),
            pltpu.VMEM((width, mix), bf16),
            pltpu.VMEM((1, mix), f32),
            pltpu.VMEM((mix, width), bf16),
            pltpu.VMEM((width, width), bf16),
            pltpu.VMEM((rows, mix), f32),
            pltpu.VMEM((N, rows, mix), f32),
            pltpu.VMEM((rows, width), f32),
            pltpu.VMEM((E, rows, mix), bf16),
            pltpu.VMEM((E, rows, mix), bf16),
            pltpu.SemaphoreType.DMA((9,)),
            pltpu.SemaphoreType.DMA((N,)),
            pltpu.SemaphoreType.DMA((N,)),
            pltpu.SemaphoreType.DMA((E,)),
            pltpu.SemaphoreType.DMA((E,)),
        ],
        compiler_params=pltpu.CompilerParams(collective_id=0, has_side_effects=True),
    )(x, in_gain[None], lw, rw, lg, rg, mid_gain[None], ow, og)
    out = out.reshape(R // IT, C, IT, width).transpose(0, 2, 1, 3)
    return out.reshape(R, C, width)


def solution(mesh):
    weight = P("trial", None)
    return jax.shard_map(
        functools.partial(local, mesh.shape["north"], mesh.shape["east"]),
        mesh=mesh,
        in_specs=(
            P(("trial", "north"), "east", None),
            P(), weight, weight, weight, weight, P(), weight, weight,
        ),
        out_specs=P(("trial", "north"), "east", None),
        check_vma=False,
    )
```

```python
import functools
import math

import jax
import jax.numpy as jnp
from jax import lax
from jax.experimental import pallas as pl
from jax.experimental.pallas import tpu as pltpu
from jax.sharding import PartitionSpec as P

MESH = pl.DeviceIdType.MESH


def norm_channels(values, gain):
    centred = values - jnp.mean(values, axis=-1, keepdims=True)
    return centred * lax.rsqrt(jnp.mean(centred * centred, axis=-1, keepdims=True) + 1e-05) * gain


def logistic(values):
    return 0.5 * jnp.tanh(0.5 * values) + 0.5


def dot(a, b):
    return jnp.dot(a, b, preferred_element_type=jnp.float32)


def tile_of(size, step, most):
    return max(t for t in range(step, most + 1, step) if size % t == 0)


def loop(count, body):
    if count == 1:
        body(0)
    else:
        pl.loop(0, count)(body)


def kernel(
    sizes,
    x_hbm, in_gain_hbm, lw_hbm, rw_hbm, lg_hbm, rg_hbm, mid_gain_hbm, ow_hbm, og_hbm,
    out_ref,
    x, in_gain, lw, rw, lg, rg, mid_gain, ow, og,
    left, right, gate, total, packed, lines, pieces, sent, got, right_sent, right_got,
    load_sem, sent_sem, got_sem, right_sent_sem, right_got_sem,
):
    N, E, R, C, IT, JT = sizes
    S = min(R, C)
    T = R // C
    rows = R * C
    block = IT * JT
    n = lax.axis_index("north")
    e = lax.axis_index("east")

    barrier = pltpu.get_barrier_semaphore()
    for far in reversed(range(1, N * E)):
        pl.semaphore_signal(
            barrier, inc=1,
            device_id={"north": lax.rem(n + far // E, N), "east": lax.rem(e + far % E, E)},
            device_id_type=MESH,
        )

    loads = [
        pltpu.make_async_copy(src, dst, load_sem.at[at])
        for at, (src, dst) in enumerate(
            (
                (x_hbm, x), (in_gain_hbm, in_gain), (lw_hbm, lw), (lg_hbm, lg), (rw_hbm, rw),
                (rg_hbm, rg), (og_hbm, og), (mid_gain_hbm, mid_gain), (ow_hbm, ow),
            )
        )
    ]
    for load in loads:
        load.start()
    for load in loads:
        load.wait()

    def own(at):
        at_rows = pl.ds(pl.multiple_of(at * block, block), block)
        ready = norm_channels(x[at_rows, :].astype(jnp.float32), in_gain[...]).astype(jnp.bfloat16)
        left[at_rows, :] = dot(ready, lw[...]) * logistic(dot(ready, lg[...]))
        right[at_rows, :] = dot(ready, rw[...]) * logistic(dot(ready, rg[...]))
        gate[at_rows, :] = logistic(dot(ready, og[...]))
        sent[T, at_rows, :] = left[at_rows, :].astype(jnp.bfloat16)
        if S == R:
            right_sent[0, at_rows, :] = right[at_rows, :].astype(jnp.bfloat16)

    loop(rows // block, own)

    if S < R:
        for t in range(T):
            for k in range(C):
                packed[pl.ds(k * S, S), :] = right[pl.ds(k * R + t * S, S), :]
            right_sent[t] = packed[...].astype(jnp.bfloat16)

    def sums_of(left_ref, i, right_ref, stride, j):
        def step(k, sums):
            lanes = left_ref[pl.ds(pl.multiple_of(k * R + i, 8), IT), :]
            return tuple(
                sums[a] + lanes * right_ref[pl.ds(k * stride + j + a, 1), :] for a in range(JT)
            )

        zeros = jnp.zeros((IT, left_ref.shape[1]), jnp.float32)
        return jnp.concatenate(lax.fori_loop(0, C, step, (zeros,) * JT, unroll=2), axis=0)

    for t in range(T):
        def tile(at):
            it, jt = at // (C // JT), at % (C // JT)
            at_rows = pl.ds(pl.multiple_of(at * block, block), block)
            sums = sums_of(left, it * IT, right, R, t * C + jt * JT)

            @pl.when(n * T + t == e)
            def _():
                total[at_rows, :] = sums

            sent[t, at_rows, :] = sums.astype(jnp.bfloat16)

        loop(rows // block, tile)

    pl.semaphore_wait(barrier, N * E - 1)

    def right_copy(t, p, target_north, target_east, source_east):
        return pltpu.make_async_remote_copy(
            right_sent.at[t], right_got.at[p, source_east],
            right_sent_sem.at[t, lax.rem(target_north + N - n, N)], right_got_sem.at[p, source_east],
            device_id={"north": target_north, "east": target_east}, device_id_type=MESH,
        )

    def right_copies(act):
        for t in range(R // S):
            piece = n * (R // S) + t
            target, p = piece // (C // S), lax.rem(piece, C // S)
            for d in reversed(range(1, N)):
                act(right_copy(t, p, lax.rem(n + d, N), target, e))
            if T == 0:
                @pl.when(target != e)
                def _():
                    act(right_copy(t, p, n, target, e))

    def got_copy(slot, peer, source):
        return pltpu.make_async_remote_copy(
            sent.at[slot], got.at[source], sent_sem.at[peer], got_sem.at[source],
            device_id={"east": peer}, device_id_type=MESH,
        )

    def got_copies(act):
        for d in range(1, E):
            peer = lax.rem(e + d, E)
            slot = T
            if T:
                slot = jnp.where(peer // T == n, lax.rem(peer, T), T)
            act(got_copy(slot, peer, e))

    right_copies(lambda copy: copy.start())
    got_copies(lambda copy: copy.start())

    order = [sorted(range(E), key=lambda s: (abs(s - v), s)) for v in range(E)]
    sources = [sum(jnp.where(e == v, order[v][d], 0) for v in range(E)) for d in range(E)]

    def add_tiles():
        for source in sources[1:]:
            got_copy(T, source, source).wait_recv()

            def add(at):
                at_rows = pl.ds(pl.multiple_of(at * block, block), block)
                total[at_rows, :] += got[source, at_rows, :].astype(jnp.float32)

            loop(rows // block, add)

    def multiply_lines():
        for d, source in enumerate(sources):
            if d:
                got_copy(T, source, source).wait_recv()

                def widen(at):
                    at_rows = pl.ds(pl.multiple_of(at * block, block), block)
                    lines[at_rows, :] = got[source, at_rows, :].astype(jnp.float32)

                loop(rows // block, widen)
            for p in range(C // S):
                owner = (e * (C // S) + p) // (R // S)

                def widen_piece(ref):
                    def widen(at):
                        at_rows = pl.ds(pl.multiple_of(at * C * JT, C * JT), C * JT)
                        pieces[at_rows, :] = ref[at_rows, :].astype(jnp.float32)

                    loop(S // JT, widen)

                if d == 0 and T == 0:
                    @pl.when(owner == n)
                    def _():
                        widen_piece(right_sent.at[0])

                    @pl.when(owner != n)
                    def _():
                        right_copy(0, p, owner, e, source).wait_recv()
                        widen_piece(right_got.at[p, source])
                else:
                    right_copy(0, p, owner, e, source).wait_recv()
                    widen_piece(right_got.at[p, source])

                def multiply(at):
                    it, jt = at // (S // JT), at % (S // JT)
                    to = it * (C // JT) + p * (S // JT) + jt
                    at_rows = pl.ds(pl.multiple_of(to * block, block), block)
                    sums = sums_of(left if d == 0 else lines, it * IT, pieces, S, jt * JT)
                    if d:
                        sums += total[at_rows, :]
                    total[at_rows, :] = sums

                loop((R // IT) * (S // JT), multiply)

    if T:
        pl.when(e // T == n)(add_tiles)
        pl.when(e // T != n)(multiply_lines)
    else:
        multiply_lines()

    def finish(at):
        start = pl.multiple_of(at * block, block)
        mixed = (total[pl.ds(start, block), :] * (C * E) ** (-0.5)).astype(jnp.bfloat16)
        scaled = norm_channels(mixed.astype(jnp.float32), mid_gain[...]).astype(jnp.bfloat16)
        it, jt = at // (C // JT), at % (C // JT)
        gates = jnp.concatenate(
            [gate[pl.ds(pl.multiple_of((jt * JT + a) * R + it * IT, 8), IT), :] for a in range(JT)],
            axis=0,
        )
        out_ref[pl.ds(start, block), :] = (dot(scaled, ow[...]) * gates).astype(jnp.bfloat16)

    loop(rows // block, finish)
    right_copies(lambda copy: copy.wait_send())
    got_copies(lambda copy: copy.wait_send())


def local(N, E, pair_state, in_gain, lw, rw, lg, rg, mid_gain, ow, og):
    R, C, width = pair_state.shape
    mix = lw.shape[1]
    S, T = min(R, C), R // C
    IT = tile_of(R, 8, 24)
    JT = tile_of(math.gcd(R, C), 1, 12)
    rows = R * C
    x = pair_state.transpose(1, 0, 2).reshape(rows, width)
    f32, bf16 = jnp.float32, jnp.bfloat16
    dma = pltpu.SemaphoreType.DMA
    out = pl.pallas_call(
        functools.partial(kernel, (N, E, R, C, IT, JT)),
        out_shape=pltpu.VMEM((rows, width), bf16),
        in_specs=[pl.BlockSpec(memory_space=pl.ANY)] * 9,
        out_specs=pl.BlockSpec(memory_space=pltpu.VMEM),
        scratch_shapes=[
            pltpu.VMEM((rows, width), bf16),
            pltpu.VMEM((1, width), f32),
            pltpu.VMEM((width, mix), bf16),
            pltpu.VMEM((width, mix), bf16),
            pltpu.VMEM((width, mix), bf16),
            pltpu.VMEM((width, mix), bf16),
            pltpu.VMEM((1, mix), f32),
            pltpu.VMEM((mix, width), bf16),
            pltpu.VMEM((width, width), bf16),
            pltpu.VMEM((rows, mix), f32),
            pltpu.VMEM((rows, mix), f32),
            pltpu.VMEM((rows, width), f32),
            pltpu.VMEM((rows, mix), f32),
            pltpu.VMEM((C * S, mix), f32),
            pltpu.VMEM((rows, mix), f32),
            pltpu.VMEM((C * S, mix), f32),
            pltpu.VMEM((T + 1, rows, mix), bf16),
            pltpu.VMEM((E, rows, mix), bf16),
            pltpu.VMEM((R // S, C * S, mix), bf16),
            pltpu.VMEM((C // S, E, C * S, mix), bf16),
            dma((9,)),
            dma((E,)),
            dma((E,)),
            dma((R // S, N)),
            dma((C // S, E)),
        ],
        compiler_params=pltpu.CompilerParams(collective_id=0, has_side_effects=True),
    )(x, in_gain[None], lw, rw, lg, rg, mid_gain[None], ow, og)
    out = out.reshape(R // IT, C, IT, width).transpose(0, 2, 1, 3)
    return out.reshape(R, C, width)


def solution(mesh):
    weight = P("trial", None)
    return jax.shard_map(
        functools.partial(local, mesh.shape["north"], mesh.shape["east"]),
        mesh=mesh,
        in_specs=(
            P(("trial", "north"), "east", None),
            P(), weight, weight, weight, weight, P(), weight, weight,
        ),
        out_specs=P(("trial", "north"), "east", None),
        check_vma=False,
    )
```

```python
import functools
import math

import jax
import jax.numpy as jnp
from jax import lax
from jax.experimental import pallas as pl
from jax.experimental.pallas import tpu as pltpu
from jax.sharding import PartitionSpec as P

MESH = pl.DeviceIdType.MESH


def norm_channels(values, gain):
    centred = values - jnp.mean(values, axis=-1, keepdims=True)
    return centred * lax.rsqrt(jnp.mean(centred * centred, axis=-1, keepdims=True) + 1e-05) * gain


def logistic(values):
    return 0.5 * jnp.tanh(0.5 * values) + 0.5


def dot(a, b):
    return jnp.dot(a, b, preferred_element_type=jnp.float32)


def tile_of(size, step, most):
    return max(t for t in range(step, most + 1, step) if size % t == 0)


def loop(count, body):
    if count == 1:
        body(0)
    else:
        pl.loop(0, count)(body)


def kernel(
    sizes,
    x_hbm, in_gain_hbm, lw_hbm, rw_hbm, lg_hbm, rg_hbm, mid_gain_hbm, ow_hbm, og_hbm,
    out_ref,
    x, in_gain, lw, rw, lg, rg, mid_gain, ow, og,
    left, right, gate, packed, pieces, sent, got, right_sent, right_got,
    load_sem, sent_sem, got_sem, right_sent_sem, right_got_sem, below_sem, above_sem,
):
    N, E, R, C, IT, JT = sizes
    S = min(R, C)
    T, parts = R // S, C // S
    rows, piece_rows, block = R * C, R * S, IT * JT
    n = lax.axis_index("north")
    e = lax.axis_index("east")
    below, above = lax.max(e - 1, 0), lax.min(e + 1, E - 1)
    has_below, has_above = e > 0, e < E - 1

    def signal(sem, axis, peer):
        pl.semaphore_signal(sem, inc=1, device_id={axis: peer}, device_id_type=MESH)

    barrier = pltpu.get_barrier_semaphore()
    for d in range(1, N):
        signal(barrier, "north", lax.rem(n + d, N))
    pl.when(has_below)(lambda: signal(barrier, "east", below))
    pl.when(has_above)(lambda: signal(barrier, "east", above))

    loads = [
        pltpu.make_async_copy(src, dst, load_sem.at[at])
        for at, (src, dst) in enumerate(
            (
                (x_hbm, x), (in_gain_hbm, in_gain), (lw_hbm, lw), (lg_hbm, lg), (rw_hbm, rw),
                (rg_hbm, rg), (og_hbm, og), (mid_gain_hbm, mid_gain), (ow_hbm, ow),
            )
        )
    ]
    for load in loads:
        load.start()
    for load in loads:
        load.wait()

    def own(at):
        at_rows = pl.ds(pl.multiple_of(at * block, block), block)
        ready = norm_channels(x[at_rows, :].astype(jnp.float32), in_gain[...]).astype(jnp.bfloat16)
        right[at_rows, :] = dot(ready, rw[...]) * logistic(dot(ready, rg[...]))
        left[at_rows, :] = dot(ready, lw[...]) * logistic(dot(ready, lg[...]))
        gate[at_rows, :] = logistic(dot(ready, og[...]))
        if S == R:
            right_sent[0, at_rows, :] = right[at_rows, :].astype(jnp.bfloat16)

    loop(rows // block, own)

    if S < R:
        for t in range(T):
            for k in range(C):
                packed[pl.ds(k * S, S), :] = right[pl.ds(k * R + t * S, S), :]
            right_sent[t] = packed[...].astype(jnp.bfloat16)

    pl.semaphore_wait(
        barrier, N - 1 + has_below.astype(jnp.int32) + has_above.astype(jnp.int32)
    )

    def right_copy(d, t, peer, owner):
        return pltpu.make_async_remote_copy(
            right_sent.at[t], right_got.at[owner, t],
            right_sent_sem.at[d, t], right_got_sem.at[owner, t],
            device_id={"north": peer}, device_id_type=MESH,
        )

    def right_copies(act):
        for d in range(1, N):
            for t in range(T):
                act(right_copy(d, t, lax.rem(n + d, N), n))

    right_copies(lambda copy: copy.start())

    @pl.when(has_below & has_above)
    def _():
        signal(below_sem, "east", above)
        signal(above_sem, "east", below)

    def tile(m, t, right_ref, stride, offset):
        def one(at):
            it, jt = at // (S // JT), at % (S // JT)

            def step(k, sums):
                lanes = left[pl.ds(pl.multiple_of(k * R + it * IT, 8), IT), :]
                first = k * stride + offset + jt * JT
                return tuple(sums[a] + lanes * right_ref[pl.ds(first + a, 1), :] for a in range(JT))

            zeros = jnp.zeros((IT, left.shape[1]), jnp.float32)
            sums = lax.fori_loop(0, C, step, (zeros,) * JT, unroll=2)
            at_rows = pl.ds(pl.multiple_of(at * block, block), block)
            sent[m, t, at_rows, :] = jnp.concatenate(sums, axis=0).astype(jnp.bfloat16)

        loop(piece_rows // block, one)

    for t in range(T):
        tile(n, t, right, R, t * S)

    for k in range(2, E):
        @pl.when(e - k >= 0)
        def _():
            pl.semaphore_wait(below_sem, 1)
            pl.when(has_above)(lambda: signal(below_sem, "east", above))

        @pl.when(e + k < E)
        def _():
            pl.semaphore_wait(above_sem, 1)
            pl.when(has_below)(lambda: signal(above_sem, "east", below))

    def got_copy(m, t, peer, source, p):
        return pltpu.make_async_remote_copy(
            sent.at[m, t], got.at[source, p], sent_sem.at[m, t], got_sem.at[source, p],
            device_id={"east": peer}, device_id_type=MESH,
        )

    def send(m, act):
        for t in range(T):
            target, p = (m * T + t) // parts, lax.rem(m * T + t, parts)

            @pl.when(target != e)
            def _():
                act(got_copy(m, t, target, e, p))

    send(n, lambda copy: copy.start())

    for d in range(1, N):
        m = lax.rem(n + N - d, N)
        for t in range(T):
            right_copy(d, t, m, m).wait_recv()

            def widen(at):
                at_rows = pl.ds(pl.multiple_of(at * C * JT, C * JT), C * JT)
                pieces[at_rows, :] = right_got[m, t, at_rows, :].astype(jnp.float32)

            loop(S // JT, widen)
            tile(m, t, pieces, S, 0)
            target, p = (m * T + t) // parts, lax.rem(m * T + t, parts)

            @pl.when(target != e)
            def _():
                got_copy(m, t, target, e, p).start()

    for d in range(1, E):
        source = lax.rem(e + d, E)
        for p in range(parts):
            got_copy(0, 0, source, source, p).wait_recv()

    for p in range(parts):
        piece = e * parts + p
        own_north, own_piece = piece // T, lax.rem(piece, T)

        def finish(at):
            at_rows = pl.ds(pl.multiple_of(at * block, block), block)
            total = sent[own_north, own_piece, at_rows, :].astype(jnp.float32)
            for d in range(1, E):
                total += got[lax.rem(e + d, E), p, at_rows, :].astype(jnp.float32)
            mixed = (total * (C * E) ** (-0.5)).astype(jnp.bfloat16)
            scaled = norm_channels(mixed.astype(jnp.float32), mid_gain[...]).astype(jnp.bfloat16)
            it, jt = at // (S // JT), at % (S // JT)
            first = (p * S + jt * JT) * R + it * IT
            gates = jnp.concatenate(
                [gate[pl.ds(pl.multiple_of(first + a * R, 8), IT), :] for a in range(JT)], axis=0
            )
            out_rows = pl.ds(pl.multiple_of(p * piece_rows + at * block, block), block)
            out_ref[out_rows, :] = (dot(scaled, ow[...]) * gates).astype(jnp.bfloat16)

        loop(piece_rows // block, finish)

    right_copies(lambda copy: copy.wait_send())
    for m in range(N):
        send(lax.rem(n + m, N), lambda copy: copy.wait_send())


def local(N, E, pair_state, in_gain, lw, rw, lg, rg, mid_gain, ow, og):
    R, C, width = pair_state.shape
    mix = lw.shape[1]
    S = min(R, C)
    T, parts = R // S, C // S
    IT = tile_of(R, 8, 24)
    JT = tile_of(math.gcd(R, C), 1, 12)
    rows = R * C
    x = pair_state.transpose(1, 0, 2).reshape(rows, width)
    f32, bf16 = jnp.float32, jnp.bfloat16
    dma = pltpu.SemaphoreType.DMA
    out = pl.pallas_call(
        functools.partial(kernel, (N, E, R, C, IT, JT)),
        out_shape=pltpu.VMEM((rows, width), bf16),
        in_specs=[pl.BlockSpec(memory_space=pl.ANY)] * 9,
        out_specs=pl.BlockSpec(memory_space=pltpu.VMEM),
        scratch_shapes=[
            pltpu.VMEM((rows, width), bf16),
            pltpu.VMEM((1, width), f32),
            pltpu.VMEM((width, mix), bf16),
            pltpu.VMEM((width, mix), bf16),
            pltpu.VMEM((width, mix), bf16),
            pltpu.VMEM((width, mix), bf16),
            pltpu.VMEM((1, mix), f32),
            pltpu.VMEM((mix, width), bf16),
            pltpu.VMEM((width, width), bf16),
            pltpu.VMEM((rows, mix), f32),
            pltpu.VMEM((rows, mix), f32),
            pltpu.VMEM((rows, width), f32),
            pltpu.VMEM((C * S, mix), f32),
            pltpu.VMEM((C * S, mix), f32),
            pltpu.VMEM((N, T, R * S, mix), bf16),
            pltpu.VMEM((E, parts, R * S, mix), bf16),
            pltpu.VMEM((T, C * S, mix), bf16),
            pltpu.VMEM((N, T, C * S, mix), bf16),
            dma((9,)),
            dma((N, T)),
            dma((E, parts)),
            dma((N, T)),
            dma((N, T)),
            pltpu.SemaphoreType.REGULAR,
            pltpu.SemaphoreType.REGULAR,
        ],
        compiler_params=pltpu.CompilerParams(collective_id=0, has_side_effects=True),
    )(x, in_gain[None], lw, rw, lg, rg, mid_gain[None], ow, og)
    out = out.reshape(parts, R // IT, S, IT, width).transpose(1, 3, 0, 2, 4)
    return out.reshape(R, C, width)


def solution(mesh):
    weight = P("trial", None)
    return jax.shard_map(
        functools.partial(local, mesh.shape["north"], mesh.shape["east"]),
        mesh=mesh,
        in_specs=(
            P(("trial", "north"), "east", None),
            P(), weight, weight, weight, weight, P(), weight, weight,
        ),
        out_specs=P(("trial", "north"), "east", None),
        check_vma=False,
    )
```

```python
import functools
import math

import jax
import jax.numpy as jnp
from jax import lax
from jax.experimental import pallas as pl
from jax.experimental.pallas import tpu as pltpu
from jax.sharding import PartitionSpec as P

MESH = pl.DeviceIdType.MESH


def norm_channels(values, gain):
    centred = values - jnp.mean(values, axis=-1, keepdims=True)
    return centred * lax.rsqrt(jnp.mean(centred * centred, axis=-1, keepdims=True) + 1e-05) * gain


def logistic(values):
    return 0.5 * jnp.tanh(0.5 * values) + 0.5


def dot(a, b):
    return jnp.dot(a, b, preferred_element_type=jnp.float32)


def tile_of(size, step, most):
    return max(t for t in range(step, most + 1, step) if size % t == 0)


def loop(count, body):
    if count == 1:
        body(0)
    else:
        pl.loop(0, count)(body)


def kernel(
    sizes,
    x_hbm, in_gain_hbm, lw_hbm, rw_hbm, lg_hbm, rg_hbm, mid_gain_hbm, ow_hbm, og_hbm,
    out_ref,
    x, in_gain, lw, rw, lg, rg, mid_gain, ow, og,
    ready, left, right, gate, packed, pieces, sent, got, right_sent, right_got,
    load_sem, sent_sem, got_sem, right_sent_sem, right_got_sem, below_sem, above_sem,
):
    N, E, R, C, IT, JT = sizes
    S = min(R, C)
    T, parts = R // S, C // S
    rows, piece_rows, block = R * C, R * S, IT * JT
    n = lax.axis_index("north")
    e = lax.axis_index("east")
    below, above = lax.max(e - 1, 0), lax.min(e + 1, E - 1)
    has_below, has_above = e > 0, e < E - 1

    def signal(sem, axis, peer):
        pl.semaphore_signal(sem, inc=1, device_id={axis: peer}, device_id_type=MESH)

    barrier = pltpu.get_barrier_semaphore()
    for d in range(1, N):
        signal(barrier, "north", lax.rem(n + d, N))
    pl.when(has_below)(lambda: signal(barrier, "east", below))
    pl.when(has_above)(lambda: signal(barrier, "east", above))

    loads = [
        pltpu.make_async_copy(src, dst, load_sem.at[at])
        for at, (src, dst) in enumerate(
            (
                (x_hbm, x), (in_gain_hbm, in_gain), (rw_hbm, rw), (rg_hbm, rg), (lw_hbm, lw),
                (lg_hbm, lg), (og_hbm, og), (mid_gain_hbm, mid_gain), (ow_hbm, ow),
            )
        )
    ]
    for load in loads:
        load.start()
    for load in loads[:4]:
        load.wait()

    def make_right(at):
        at_rows = pl.ds(pl.multiple_of(at * block, block), block)
        normed = norm_channels(x[at_rows, :].astype(jnp.float32), in_gain[...]).astype(jnp.bfloat16)
        ready[at_rows, :] = normed
        right[at_rows, :] = dot(normed, rw[...]) * logistic(dot(normed, rg[...]))
        if S == R:
            right_sent[0, at_rows, :] = right[at_rows, :].astype(jnp.bfloat16)

    loop(rows // block, make_right)

    if S < R:
        for t in range(T):
            for k in range(C):
                packed[pl.ds(k * S, S), :] = right[pl.ds(k * R + t * S, S), :]
            right_sent[t] = packed[...].astype(jnp.bfloat16)

    pl.semaphore_wait(
        barrier, N - 1 + has_below.astype(jnp.int32) + has_above.astype(jnp.int32)
    )

    def right_copy(d, t, peer, owner):
        return pltpu.make_async_remote_copy(
            right_sent.at[t], right_got.at[owner, t],
            right_sent_sem.at[d, t], right_got_sem.at[owner, t],
            device_id={"north": peer}, device_id_type=MESH,
        )

    def right_copies(act):
        for d in range(1, N):
            for t in range(T):
                act(right_copy(d, t, lax.rem(n + d, N), n))

    right_copies(lambda copy: copy.start())

    @pl.when(has_below & has_above)
    def _():
        signal(below_sem, "east", above)
        signal(above_sem, "east", below)

    for load in loads[4:]:
        load.wait()

    def make_left(at):
        at_rows = pl.ds(pl.multiple_of(at * block, block), block)
        normed = ready[at_rows, :]
        left[at_rows, :] = dot(normed, lw[...]) * logistic(dot(normed, lg[...]))

    def make_gate(at):
        at_rows = pl.ds(pl.multiple_of(at * block, block), block)
        gate[at_rows, :] = logistic(dot(ready[at_rows, :], og[...]))

    loop(rows // block, make_left)

    def tile(m, t, right_ref, stride, offset):
        def one(at):
            it, jt = at // (S // JT), at % (S // JT)

            def step(k, sums):
                lanes = left[pl.ds(pl.multiple_of(k * R + it * IT, 8), IT), :]
                first = k * stride + offset + jt * JT
                return tuple(sums[a] + lanes * right_ref[pl.ds(first + a, 1), :] for a in range(JT))

            zeros = jnp.zeros((IT, left.shape[1]), jnp.float32)
            sums = lax.fori_loop(0, C, step, (zeros,) * JT, unroll=4)
            at_rows = pl.ds(pl.multiple_of(at * block, block), block)
            sent[m, t, at_rows, :] = jnp.concatenate(sums, axis=0).astype(jnp.bfloat16)

        loop(piece_rows // block, one)

    for t in range(T):
        tile(n, t, right, R, t * S)

    for k in range(2, E):
        @pl.when(e - k >= 0)
        def _():
            pl.semaphore_wait(below_sem, 1)
            pl.when(has_above)(lambda: signal(below_sem, "east", above))

        @pl.when(e + k < E)
        def _():
            pl.semaphore_wait(above_sem, 1)
            pl.when(has_below)(lambda: signal(above_sem, "east", below))

    def got_copy(m, t, peer, source, p):
        return pltpu.make_async_remote_copy(
            sent.at[m, t], got.at[source, p], sent_sem.at[m, t], got_sem.at[source, p],
            device_id={"east": peer}, device_id_type=MESH,
        )

    def send(m, act):
        for t in range(T):
            target, p = (m * T + t) // parts, lax.rem(m * T + t, parts)

            @pl.when(target != e)
            def _():
                act(got_copy(m, t, target, e, p))

    send(n, lambda copy: copy.start())

    loop(rows // block, make_gate)
    for d in range(1, N):
        m = lax.rem(n + N - d, N)
        for t in range(T):
            right_copy(d, t, m, m).wait_recv()

            def widen(at):
                at_rows = pl.ds(pl.multiple_of(at * C * JT, C * JT), C * JT)
                pieces[at_rows, :] = right_got[m, t, at_rows, :].astype(jnp.float32)

            loop(S // JT, widen)
            tile(m, t, pieces, S, 0)
            target, p = (m * T + t) // parts, lax.rem(m * T + t, parts)

            @pl.when(target != e)
            def _():
                got_copy(m, t, target, e, p).start()

    for d in range(1, E):
        source = lax.rem(e + d, E)
        for p in range(parts):
            got_copy(0, 0, source, source, p).wait_recv()

    for p in range(parts):
        piece = e * parts + p
        own_north, own_piece = piece // T, lax.rem(piece, T)

        def finish(at):
            at_rows = pl.ds(pl.multiple_of(at * block, block), block)
            total = sent[own_north, own_piece, at_rows, :].astype(jnp.float32)
            for d in range(1, E):
                total += got[lax.rem(e + d, E), p, at_rows, :].astype(jnp.float32)
            mixed = (total * (C * E) ** (-0.5)).astype(jnp.bfloat16)
            scaled = norm_channels(mixed.astype(jnp.float32), mid_gain[...]).astype(jnp.bfloat16)
            it, jt = at // (S // JT), at % (S // JT)
            first = (p * S + jt * JT) * R + it * IT
            gates = jnp.concatenate(
                [gate[pl.ds(pl.multiple_of(first + a * R, 8), IT), :] for a in range(JT)], axis=0
            )
            out_rows = pl.ds(pl.multiple_of(p * piece_rows + at * block, block), block)
            out_ref[out_rows, :] = (dot(scaled, ow[...]) * gates).astype(jnp.bfloat16)

        loop(piece_rows // block, finish)

    right_copies(lambda copy: copy.wait_send())
    for m in range(N):
        send(lax.rem(n + m, N), lambda copy: copy.wait_send())


def local(N, E, pair_state, in_gain, lw, rw, lg, rg, mid_gain, ow, og):
    R, C, width = pair_state.shape
    mix = lw.shape[1]
    S = min(R, C)
    T, parts = R // S, C // S
    IT = tile_of(R, 8, 24)
    JT = tile_of(math.gcd(R, C), 1, 12)
    rows = R * C
    x = pair_state.transpose(1, 0, 2).reshape(rows, width)
    f32, bf16 = jnp.float32, jnp.bfloat16
    dma = pltpu.SemaphoreType.DMA
    out = pl.pallas_call(
        functools.partial(kernel, (N, E, R, C, IT, JT)),
        out_shape=pltpu.VMEM((rows, width), bf16),
        in_specs=[pl.BlockSpec(memory_space=pl.ANY)] * 9,
        out_specs=pl.BlockSpec(memory_space=pltpu.VMEM),
        scratch_shapes=[
            pltpu.VMEM((rows, width), bf16),
            pltpu.VMEM((1, width), f32),
            pltpu.VMEM((width, mix), bf16),
            pltpu.VMEM((width, mix), bf16),
            pltpu.VMEM((width, mix), bf16),
            pltpu.VMEM((width, mix), bf16),
            pltpu.VMEM((1, mix), f32),
            pltpu.VMEM((mix, width), bf16),
            pltpu.VMEM((width, width), bf16),
            pltpu.VMEM((rows, width), bf16),
            pltpu.VMEM((rows, mix), f32),
            pltpu.VMEM((rows, mix), f32),
            pltpu.VMEM((rows, width), f32),
            pltpu.VMEM((C * S, mix), f32),
            pltpu.VMEM((C * S, mix), f32),
            pltpu.VMEM((N, T, R * S, mix), bf16),
            pltpu.VMEM((E, parts, R * S, mix), bf16),
            pltpu.VMEM((T, C * S, mix), bf16),
            pltpu.VMEM((N, T, C * S, mix), bf16),
            dma((9,)),
            dma((N, T)),
            dma((E, parts)),
            dma((N, T)),
            dma((N, T)),
            pltpu.SemaphoreType.REGULAR,
            pltpu.SemaphoreType.REGULAR,
        ],
        compiler_params=pltpu.CompilerParams(collective_id=0, has_side_effects=True),
    )(x, in_gain[None], lw, rw, lg, rg, mid_gain[None], ow, og)
    out = out.reshape(parts, R // IT, S, IT, width).transpose(1, 3, 0, 2, 4)
    return out.reshape(R, C, width)


def solution(mesh):
    weight = P("trial", None)
    return jax.shard_map(
        functools.partial(local, mesh.shape["north"], mesh.shape["east"]),
        mesh=mesh,
        in_specs=(
            P(("trial", "north"), "east", None),
            P(), weight, weight, weight, weight, P(), weight, weight,
        ),
        out_specs=P(("trial", "north"), "east", None),
        check_vma=False,
    )
```
